32 devices in a mesh: groups: 2 (over y), expert: 4 (over z), tensor: 4 (over x, core).
Axes of the slice: x: 2, y: 2, z: 4, core: 2. Of those that a mesh axis runs over, the one named last changes fastest.
Arguments:
- resid: bfloat16 [256, 3072], P(('groups', 'expert', 'tensor')), parts along dimension 0, may hold values from -6 to 6
- attn_part: bfloat16 [256, 12288], P(('groups', 'expert'), 'tensor'), parts along dimension 0, may hold values from -2 to 2
- norm_gain: float32 [3072], replicated, may hold values from 0.1 to 1.9
- w_router: bfloat16 [3072, 8], replicated, may hold values from -0.3125 to 0.3125
- routes: int32 [256, 2], P(('groups', 'expert', 'tensor')), parts along dimension 0, may hold values from 0 to 7, all different within a row; in each aligned block of 8 rows (0 to 7, 8 to 15, ...) at most 4 rows name the same one
- w_gate: bfloat16 [3072, 65536], P(None, ('expert', 'tensor')), may hold values from -0.109375 to 0.109375
- w_up: bfloat16 [3072, 65536], P(None, ('expert', 'tensor')), may hold values from -0.109375 to 0.109375
- w_down: bfloat16 [65536, 3072], P(('expert', 'tensor')), may hold values from -0.0625 to 0.0625
Outputs:
- block_out: bfloat16 [256, 3072], P(('groups', 'expert', 'tensor')), parts along dimension 0
The draws below stay inside these ranges and needn't reach their ends.
There are 2 independent parts, one for each index of `groups`. The reference program is written for one: setup_inputs(seed, part) draws one part's arguments, and reference() takes and returns one part's arrays. A program takes and returns all parts, laid end to end along the dimension named above; an argument that names none is the same for every part. Nothing has to cross between parts.
Inputs may be any that keep to these rules, and one draw needn't show every extreme that they name: `routes`: the two entries of a row differ. Within the 8 rows of one device no expert is named more than 4 times, and in some device's rows some expert is named exactly 4 times.
All inputs are finite; a program needn't handle non-finite values.
Results may differ from the reference program's by a relative error of at most 0.02.
Values may be sent and summed in bfloat16 or wider, within the bound.
No kernel may reach another device: no remote copies, remote signals or barrier semaphores. Data moves between devices by JAX's collectives and lax.ppermute only.
A program may use at most 128 MiB of HBM per device.

```python
import math
import jax
import jax.numpy as jnp
import numpy as np
from jax import lax

D = 3072
FF = 8192
E = 8
TOK_DEV = 8
CAP = 4
TOKENS = 128
N_TENSOR = 4


def block_levels(key, dims, split, least, top_value):
    level, own = 1.0, jax.random.fold_in(key, 6)
    for dim, shards_of in split:
        draws = jnp.exp(jax.random.uniform(jax.random.fold_in(own, dim), (shards_of,), jnp.float32, least / len(split), top_value / len(split)))
        level = level * jnp.repeat(draws, dims[dim] // shards_of).reshape([-1 if axis == dim else 1 for axis in range(len(dims))])
    return level


def shared_out(rng, own, number, rows, amount, top, most, slope):
    sequence = jax.random.permutation(rng, amount)
    heavy_load, usual = load_shares(amount, rows * top, most, slope, True), load_shares(amount, rows * top, most, slope, False)
    places = jnp.arange(amount)

    def named(sizes, offset_by):
        used = int((sizes > 0).sum())
        fixed = max(1, used // 4)
        shifted = fixed + (places - fixed + offset_by * (used - fixed)) % max(1, amount - fixed)
        return jnp.zeros((amount,), jnp.int32).at[sequence[jnp.where(places < fixed, places, shifted)]].set(jnp.asarray(sizes, jnp.int32))

    sizes = jnp.where(number % 4 == 0, named(heavy_load, number // 4), named(usual, number - number // 4 - 1))
    mixed = jax.random.permutation(jax.random.fold_in(own, 3), amount)
    source_of, taker = mixed[0:amount // 2 * 2:2], mixed[1:amount // 2 * 2:2]
    slack = jnp.minimum(sizes[source_of] - 1, most - sizes[taker]) // 2
    slack = jnp.where((source_of == sequence[0]) | (taker == sequence[0]) | (sizes[taker] == 0), 0, jnp.maximum(slack, 0))
    shifted = jax.random.randint(jax.random.fold_in(own, 4), (amount // 2,), 0, 1 << 20) % (slack + 1)
    sizes = sizes.at[source_of].add(-shifted).at[taker].add(shifted)
    members = jnp.searchsorted(jnp.cumsum(sizes), jnp.arange(rows * top), side="right").astype(jnp.int32)
    listing = members.reshape(top, rows).T
    listing = listing[jax.random.permutation(jax.random.fold_in(own, 1), rows)]
    offset_by = jax.random.randint(jax.random.fold_in(own, 2), (rows, 1), 0, top)
    return jnp.take_along_axis(listing, (jnp.arange(top)[None, :] + offset_by) % top, axis=1)


def load_shares(amount, total, limit, skew, full):
    loads = [(1 << 20) // math.isqrt(standing ** skew) + 1 for standing in range(1, amount + 1)]
    largest = limit if full else min(limit, max(-(-total // amount), total * loads[0] // sum(loads)))
    least = 1 if total - largest >= amount - 1 else 0
    holding, spare = [largest] + [least] * (amount - 1), total - largest - least * (amount - 1)
    while spare > 0:
        movable = [i for i in range(1, amount) if holding[i] < largest] or [i for i in range(1, amount) if holding[i] < limit]
        whole, remaining = sum([loads[i] for i in movable]), spare
        for i in movable:
            more = min(limit - holding[i], max(1, remaining * loads[i] // whole), spare)
            holding[i] = holding[i] + more
            spare = spare - more
    return np.array(holding)


def normal_values(rng, shape, scale, most, shards=(), kind=jnp.bfloat16):
    loudness = block_levels(rng, shape, shards, -0.22, 0.18) if shards else 1.0
    drawn = jax.random.normal(rng, shape, jnp.float32) * scale * loudness
    return jnp.minimum(jnp.maximum(drawn, -most), most).astype(kind)


def setup_inputs(seed: int = 0, part: int = 0) -> dict:
    keys = jax.random.split(jax.random.key(seed), 9)
    part_keys = jax.random.split(jax.random.fold_in(keys[8], part), 9)
    resid = normal_values(part_keys[0], (TOKENS, D), 1.0, 6.0, ((0, 16),))
    attn_part = normal_values(part_keys[1], (TOKENS, N_TENSOR * D), 0.35, 2.0, ((0, 4), (1, 4)))
    norm_gain = jnp.clip(1.0 + 0.18 * jax.random.normal(keys[2], (D,), jnp.float32), 0.1, 1.9)
    w_router = normal_values(keys[3], (D, E), (D // 8) ** -0.5, 0.3125)
    routes_keys = jax.random.split(jax.random.fold_in(part_keys[4], 1), TOKENS // TOK_DEV)
    routes_turns = jax.random.permutation(jax.random.fold_in(part_keys[4], 3), TOKENS // TOK_DEV)
    routes = jax.vmap(lambda own, number: shared_out(jax.random.fold_in(part_keys[4], 2), own, number, TOK_DEV, E, 2, CAP, 2))(routes_keys, routes_turns).reshape((TOKENS, 2))
    w_gate = normal_values(keys[5], (D, E * FF), D ** -0.5, 0.109375, ((1, 16),))
    w_up = normal_values(keys[6], (D, E * FF), D ** -0.5, 0.109375, ((1, 16),))
    w_down = normal_values(keys[7], (E * FF, D), FF ** -0.5, 0.0625, ((0, 16),))
    return dict(resid=resid, attn_part=attn_part, norm_gain=norm_gain, w_router=w_router, routes=routes, w_gate=w_gate, w_up=w_up, w_down=w_down)


EPSILON = 1e-05

def reference(resid, attn_part, norm_gain, w_router, routes, w_gate, w_up, w_down):
    token_count = resid.shape[0]
    attn_sum = lax.optimization_barrier(jnp.sum(attn_part.astype(jnp.float32).reshape(token_count, N_TENSOR, D), axis=1))
    hidden_state = (resid.astype(jnp.float32) + attn_sum).astype(jnp.bfloat16)
    hidden_wide = lax.optimization_barrier(hidden_state).astype(jnp.float32)
    inverse_rms = lax.rsqrt(lax.optimization_barrier(jnp.mean(hidden_wide * hidden_wide, axis=1, keepdims=True)) + EPSILON)
    normed = (hidden_wide * inverse_rms * norm_gain.astype(jnp.float32)).astype(jnp.bfloat16)
    logits = jnp.dot(normed, w_router, preferred_element_type=jnp.float32)
    first_logit = jnp.take_along_axis(logits, routes[:, 0:1], axis=1)[:, 0]
    second_logit = jnp.take_along_axis(logits, routes[:, 1:2], axis=1)[:, 0]
    share_first = jax.nn.sigmoid(first_logit - second_logit)
    share_second = 1.0 - share_first
    expert_range = jnp.arange(E, dtype=jnp.int32)
    per_token = lax.optimization_barrier(jnp.sum((routes[:, :, None] == expert_range).astype(jnp.int32), axis=1))
    block_count = token_count // TOK_DEV
    blocked = per_token.reshape(block_count, TOK_DEV, E)
    running = (jnp.cumsum(blocked, axis=1) - blocked).reshape(token_count, E).astype(jnp.int32)
    block_index = jnp.arange(token_count, dtype=jnp.int32) // TOK_DEV
    column_count = block_count * CAP
    targets = []
    for pick_index in range(2):
        chosen = routes[:, pick_index]
        slot_index = jnp.take_along_axis(running, routes[:, pick_index:pick_index + 1], axis=1)[:, 0]
        targets.append((chosen * column_count + block_index * CAP + slot_index).astype(jnp.int32))
    expert_input = jnp.zeros((E * column_count, D), jnp.bfloat16)
    expert_input = expert_input.at[targets[0]].set(normed).at[targets[1]].set(normed)
    expert_input = expert_input.reshape(E, column_count, D)

    def run_expert(operands):
        expert_id, inputs = operands
        gate_cols = lax.dynamic_slice_in_dim(w_gate, expert_id * FF, FF, 1)
        up_cols = lax.dynamic_slice_in_dim(w_up, expert_id * FF, FF, 1)
        down_rows = lax.dynamic_slice_in_dim(w_down, expert_id * FF, FF, 0)
        gate_value = jnp.dot(inputs, gate_cols, preferred_element_type=jnp.float32)
        up_value = jnp.dot(inputs, up_cols, preferred_element_type=jnp.float32)
        activated = (jax.nn.silu(gate_value) * up_value).astype(jnp.bfloat16)
        return jnp.dot(activated, down_rows, preferred_element_type=jnp.float32)
    expert_output = lax.map(run_expert, (expert_range, expert_input)).reshape(E * column_count, D)
    mixed = hidden_wide + share_first[:, None] * expert_output[targets[0]] + share_second[:, None] * expert_output[targets[1]]
    return mixed.astype(jnp.bfloat16)
```

```python
import functools
import jax
import jax.numpy as jnp
from jax import lax
from jax.experimental import pallas as pl
from jax.experimental.pallas import tpu as pltpu
from jax.sharding import PartitionSpec as P

E = 8


EPSILON = 1e-05
SMALL = 6 << 20


def partner(shard, axis, distance):
    return lax.ppermute(shard, axis, [(i, i ^ 1 << distance) for i in range(lax.axis_size(axis))])


def flip(shard, axis, mask):
    return lax.ppermute(shard, axis, [(i, i ^ mask) for i in range(lax.axis_size(axis))])


def whole():
    return pl.BlockSpec(memory_space=pltpu.VMEM)


def small_call(kernel, outs, name, flops=1 << 20):
    return pl.pallas_call(
        kernel,
        out_shape=outs,
        out_specs=jax.tree.map(lambda _: whole(), outs),
        compiler_params=pltpu.CompilerParams(vmem_limit_bytes=SMALL),
        cost_estimate=pl.CostEstimate(flops=flops, bytes_accessed=1 << 18, transcendentals=0),
        name=name,
    )


def chip_sum_kernel(own_ref, got_ref, resid_ref, pick_ref, sum_ref, send_ref):
    tensor = lax.axis_index("tensor")
    core, column = tensor % 2, tensor // 2
    rows, features = resid_ref.shape
    for side in range(2):
        take = pl.ds(pl.multiple_of((2 * side + core) * rows, rows), rows)
        total = own_ref[take, :].astype(jnp.float32) + got_ref[take, :].astype(jnp.float32)
        mine = (column == side).astype(jnp.float32)
        total = total + mine * resid_ref[...].astype(jnp.float32)
        sum_ref[side * rows : (side + 1) * rows, :] = total
    send_ref[:, :features] = sum_ref[...].astype(jnp.bfloat16)
    send_ref[:, features:] = jnp.concatenate([pick_ref[...], pick_ref[...]], axis=0)


def dispatch_kernel(capacity, sum_ref, got_ref, pick_ref, gain_ref, router_ref, weight_ref, hidden_ref, *out_refs):
    tensor = lax.axis_index("tensor")
    my_expert_rank = lax.axis_index("expert")
    column = tensor // 2
    rows, features = hidden_ref.shape
    tokens = 2 * rows
    hidden = (sum_ref[...] + got_ref[:, :features].astype(jnp.float32)).astype(jnp.bfloat16)
    wide = hidden.astype(jnp.float32)
    inverse_rms = lax.rsqrt(jnp.mean(wide * wide, axis=1, keepdims=True) + EPSILON)
    normed = (wide * inverse_rms * gain_ref[...]).astype(jnp.bfloat16)
    logits = lax.dot_general(
        normed, router_ref[...], (((1,), (1,)), ((), ())), preferred_element_type=jnp.float32
    )
    side = lax.broadcasted_iota(jnp.int32, (tokens, 1), 0) // rows
    mine = jnp.concatenate([pick_ref[...], pick_ref[...]], axis=0).astype(jnp.float32)
    theirs = got_ref[:, features:].astype(jnp.float32)
    picks = jnp.where(side == column, mine, theirs)
    first, second = picks[:, 0:1], picks[:, 1:2]
    experts = lax.broadcasted_iota(jnp.int32, (tokens, E), 1).astype(jnp.float32)
    is_first = (first == experts).astype(jnp.float32)
    is_second = (second == experts).astype(jnp.float32)
    difference = jnp.sum((is_first - is_second) * logits, axis=1, keepdims=True)
    share_first = 1.0 / (1.0 + jnp.exp(-difference))
    share_second = 1.0 - share_first
    later = lax.broadcasted_iota(jnp.int32, (tokens, tokens), 0)
    earlier = lax.broadcasted_iota(jnp.int32, (tokens, tokens), 1)
    ahead = ((later > earlier) & (later // rows == earlier // rows)).astype(jnp.float32)
    before = jnp.dot(ahead, is_first + is_second, preferred_element_type=jnp.float32)
    slot_first = jnp.sum(before * is_first, axis=1, keepdims=True)
    slot_second = jnp.sum(before * is_second, axis=1, keepdims=True)
    cell = lax.broadcasted_iota(jnp.int32, (tokens, 128), 1)
    block = 2 * capacity
    distance = cell // block
    target = (2 * (my_expert_rank ^ distance) + column).astype(jnp.float32)
    cell_slot = (cell % capacity).astype(jnp.float32)
    here = (cell // capacity % 2 == side) & (distance < len(out_refs))
    at_first = (here & (first == target) & (slot_first == cell_slot)).astype(jnp.float32)
    at_second = (here & (second == target) & (slot_second == cell_slot)).astype(jnp.float32)
    weight_ref[...] = share_first * at_first + share_second * at_second
    placement = (at_first + at_second).T.astype(jnp.bfloat16)
    outgoing = jnp.dot(
        placement[: block * len(out_refs), :], normed, preferred_element_type=jnp.float32
    ).astype(jnp.bfloat16)
    for index, out_ref in enumerate(out_refs):
        out_ref[...] = outgoing[index * block : (index + 1) * block, :]
    hidden_ref[...] = jnp.where(column == 0, wide[:rows, :], wide[rows:, :])


def expert_kernel(chunk, slots, own_ref, got_ref, gate_ref, up_ref, down_ref, keep_ref, send_ref, tokens, active, ring, sems):
    half, features = keep_ref.shape
    hidden = gate_ref.shape[1]
    pieces = features // chunk

    def fetch(index):
        return pltpu.make_async_copy(
            down_ref.at[:, pl.ds(index * chunk, chunk)], ring.at[index % slots], sems.at[index % slots]
        )

    for index in range(min(slots, pieces)):
        fetch(index).start()
    tokens[:half, :] = own_ref[...]
    tokens[half:, :] = got_ref[...]
    for index in range(hidden // chunk):
        span = slice(index * chunk, (index + 1) * chunk)
        gate = jnp.dot(tokens[...], gate_ref[:, span], preferred_element_type=jnp.float32)
        up = jnp.dot(tokens[...], up_ref[:, span], preferred_element_type=jnp.float32)
        active[:, span] = (gate / (1.0 + jnp.exp(-gate)) * up).astype(jnp.bfloat16)
    for index in range(pieces):
        span = slice(index * chunk, (index + 1) * chunk)
        fetch(index).wait()
        produced = jnp.dot(active[...], ring[index % slots], preferred_element_type=jnp.float32)
        keep_ref[:, span] = produced[:half, :]
        send_ref[:, span] = produced[half:, :].astype(jnp.bfloat16)
        if index + slots < pieces:
            fetch(index + slots).start()


def pair_sum_kernel(keep_ref, got_ref, *out_refs):
    total = (keep_ref[...] + got_ref[...].astype(jnp.float32)).astype(jnp.bfloat16)
    block = out_refs[0].shape[0]
    for index, out_ref in enumerate(out_refs):
        out_ref[...] = total[index * block : (index + 1) * block, :]


def combine_kernel(weight_ref, hidden_ref, *refs):
    blocks, keep_ref, send_ref = refs[:-2], refs[-2], refs[-1]
    column = lax.axis_index("tensor") // 2
    rows = hidden_ref.shape[0]
    returned = jnp.concatenate([ref[...] for ref in blocks], axis=0)
    weight = weight_ref[:, : returned.shape[0]]
    high = weight.astype(jnp.bfloat16)
    low = (weight - high.astype(jnp.float32)).astype(jnp.bfloat16)
    mixed = jnp.dot(high, returned, preferred_element_type=jnp.float32)
    mixed = mixed + jnp.dot(low, returned, preferred_element_type=jnp.float32)
    upper, lower = mixed[:rows, :], mixed[rows:, :]
    keep_ref[...] = hidden_ref[...] + jnp.where(column == 0, upper, lower)
    send_ref[...] = jnp.where(column == 0, lower, upper).astype(jnp.bfloat16)


def finish_kernel(keep_ref, got_ref, out_ref):
    out_ref[...] = (keep_ref[...] + got_ref[...].astype(jnp.float32)).astype(jnp.bfloat16)


def paired_shards(resid, attn_part, norm_gain, w_router, routes, w_gate, w_up, w_down):
    expert_ranks = lax.axis_size("expert")
    rows, features = resid.shape
    capacity = rows // 2
    block = 2 * capacity
    half = block * expert_ranks
    bf16, f32 = jnp.bfloat16, jnp.float32
    shape = jax.ShapeDtypeStruct
    gate = pltpu.with_memory_space_constraint(w_gate, pltpu.VMEM)
    up = pltpu.with_memory_space_constraint(w_up, pltpu.VMEM)
    picks = jnp.pad(routes.astype(bf16), ((0, 0), (0, 128 - routes.shape[1])))
    other_core = flip(attn_part, "tensor", 1)
    chip_sum, sending = small_call(
        chip_sum_kernel,
        (shape((2 * rows, features), f32), shape((2 * rows, features + 128), bf16)),
        "chip_sum",
    )(attn_part, other_core, resid, picks)
    other_column = flip(sending, "tensor", 2)
    weight, hidden, *outgoing = small_call(
        functools.partial(dispatch_kernel, capacity),
        (shape((2 * rows, 128), f32), shape((rows, features), f32))
        + (shape((block, features), bf16),) * expert_ranks,
        "dispatch",
    )(chip_sum, other_column, picks, norm_gain.reshape(1, features), w_router.T)
    arrived = [outgoing[0]] + [flip(outgoing[d], "expert", d) for d in range(1, expert_ranks)]
    own_slots = jnp.concatenate(arrived, axis=0)
    other_slots = flip(own_slots, "tensor", 1)
    chunk = 512
    slots = 3
    keep, give = pl.pallas_call(
        functools.partial(expert_kernel, chunk, slots),
        out_shape=(shape((half, features), f32), shape((half, features), bf16)),
        in_specs=[whole()] * 4 + [pl.BlockSpec(memory_space=pl.ANY)],
        out_specs=(whole(), whole()),
        scratch_shapes=[
            pltpu.VMEM((2 * half, features), bf16),
            pltpu.VMEM((2 * half, w_gate.shape[1]), bf16),
            pltpu.VMEM((slots, w_down.shape[0], chunk), bf16),
            pltpu.SemaphoreType.DMA((slots,)),
        ],
        compiler_params=pltpu.CompilerParams(vmem_limit_bytes=15 << 20),
        cost_estimate=pl.CostEstimate(
            flops=12 * half * w_gate.size // 1, bytes_accessed=3 * w_gate.size, transcendentals=0
        ),
        name="experts",
    )(own_slots, other_slots, gate, up, w_down)
    given = flip(give, "tensor", 1)
    returning = small_call(
        pair_sum_kernel, (shape((block, features), bf16),) * expert_ranks, "pair_sum"
    )(keep, given)
    returned = [returning[0]] + [flip(returning[d], "expert", d) for d in range(1, expert_ranks)]
    kept, mixed = small_call(
        combine_kernel, (shape((rows, features), f32), shape((rows, features), bf16)), "combine"
    )(weight, hidden, *returned)
    other_mixed = flip(mixed, "tensor", 2)
    return small_call(finish_kernel, shape((rows, features), bf16), "finish")(kept, other_mixed)


def shards(resid, attn_part, norm_gain, w_router, routes, w_gate, w_up, w_down):
    expert_ranks = lax.axis_size("expert")
    tensor_ranks = lax.axis_size("tensor")
    my_expert_rank = lax.axis_index("expert")
    my_tensor_rank = lax.axis_index("tensor")
    token_rows = resid.shape[0]
    feature_count = resid.shape[1]
    holders = max(1, expert_ranks // E)
    hosted = max(1, E // expert_ranks)
    expert_groups = E // hosted
    capacity = token_rows // 2
    rank_slots = hosted * capacity
    feature_share = feature_count // holders
    levels = holders.bit_length() - 1
    partial_terms = attn_part.astype(jnp.float32)
    attn_rows = lax.psum_scatter(
        partial_terms.astype(jnp.bfloat16), "tensor", scatter_dimension=0, tiled=True
    ).astype(jnp.float32)
    hidden_state = (resid.astype(jnp.float32) + attn_rows).astype(jnp.bfloat16)
    hidden_wide = lax.optimization_barrier(hidden_state).astype(jnp.float32)
    inverse_rms = lax.rsqrt(jnp.mean(hidden_wide * hidden_wide, axis=1, keepdims=True) + EPSILON)
    normed = (hidden_wide * inverse_rms * norm_gain).astype(jnp.bfloat16)
    logits = jnp.dot(normed, w_router, preferred_element_type=jnp.float32)
    expert_columns = lax.broadcasted_iota(jnp.int32, (token_rows, E), 1)
    pick_first = (routes[:, 0:1] == expert_columns).astype(jnp.float32)
    pick_second = (routes[:, 1:2] == expert_columns).astype(jnp.float32)
    share_first = jax.nn.sigmoid(jnp.sum((pick_first - pick_second) * logits, axis=1))
    share_second = 1.0 - share_first
    row_later = lax.broadcasted_iota(jnp.int32, (token_rows, token_rows), 0)
    row_earlier = lax.broadcasted_iota(jnp.int32, (token_rows, token_rows), 1)
    earlier = (row_later > row_earlier).astype(jnp.float32)
    before = jnp.dot(earlier, pick_first + pick_second, precision=lax.Precision.HIGHEST)
    slot_first = jnp.sum(before * pick_first, axis=1)
    slot_second = jnp.sum(before * pick_second, axis=1)
    slot_numbers = lax.broadcasted_iota(jnp.int32, (token_rows, E, capacity), 2).astype(jnp.float32)
    cell_first = pick_first[:, :, None] * (slot_numbers == slot_first[:, None, None]).astype(
        jnp.float32
    )
    cell_second = pick_second[:, :, None] * (slot_numbers == slot_second[:, None, None]).astype(
        jnp.float32
    )
    placement = (
        (cell_first + cell_second)
        .reshape(token_rows, expert_groups, rank_slots)
        .astype(jnp.bfloat16)
    )
    combine_weight = (
        share_first[:, None, None] * cell_first + share_second[:, None, None] * cell_second
    ).reshape(token_rows, expert_groups, rank_slots)
    outgoing = jnp.einsum(
        "rgc,rd->gcd", placement, normed, preferred_element_type=jnp.float32
    ).astype(jnp.bfloat16)
    outgoing = jnp.repeat(outgoing, holders, axis=0)
    arrived = lax.all_to_all(outgoing, "expert", split_axis=0, concat_axis=0, tiled=True)
    device_span = my_expert_rank * tensor_ranks + my_tensor_rank
    own_expert = device_span * E // (expert_ranks * tensor_ranks)
    local_index = own_expert - my_expert_rank // holders * hosted

    def activate(token_block):
        source_count = token_block.shape[0]
        selected = lax.dynamic_slice_in_dim(token_block, local_index * capacity, capacity, 1)
        flattened = selected.reshape(source_count * capacity, feature_count)
        gate_value = jnp.dot(flattened, w_gate, preferred_element_type=jnp.float32)
        up_value = jnp.dot(flattened, w_up, preferred_element_type=jnp.float32)
        return (jax.nn.silu(gate_value) * up_value).astype(jnp.bfloat16)

    def expert_partial(token_block):
        source_count = token_block.shape[0]
        activated = activate(token_block)
        produced = jnp.dot(activated, w_down, preferred_element_type=jnp.float32).reshape(
            source_count, capacity, feature_count
        )
        if hosted == 1:
            return produced
        blank = jnp.zeros((source_count, rank_slots, feature_count), jnp.float32)
        return lax.dynamic_update_slice_in_dim(blank, produced, local_index * capacity, 1)

    partial_value = expert_partial(lax.all_gather(arrived, "tensor", axis=0, tiled=True))
    leading = partial_value.shape[0]
    layered = partial_value.reshape((leading, rank_slots) + (2,) * levels + (feature_share,))
    remaining = [section for section in range(levels - 1, -1, -1)]
    for section in range(levels):
        split_axis = 2 + remaining.index(section)
        my_side = my_expert_rank // 2**section % 2
        kept_half = lax.dynamic_index_in_dim(layered, my_side, split_axis, keepdims=False)
        given_half = lax.dynamic_index_in_dim(layered, 1 - my_side, split_axis, keepdims=False)
        layered = kept_half + partner(given_half.astype(jnp.bfloat16), "expert", section).astype(
            given_half.dtype
        )
        remaining = [other for other in remaining if other != section]
    own_sources = lax.psum_scatter(
        layered.astype(jnp.bfloat16), "tensor", scatter_dimension=0, tiled=True
    ).astype(jnp.float32)
    returned = lax.all_to_all(
        own_sources.astype(jnp.bfloat16), "expert", split_axis=0, concat_axis=0, tiled=True
    ).astype(own_sources.dtype)
    returned_view = returned.reshape(expert_groups, holders, rank_slots, feature_share)
    mixed = jnp.einsum(
        "rgc,gscp->rsp", combine_weight, returned_view, precision=lax.Precision.HIGHEST
    )
    mixed = mixed.reshape(token_rows, feature_count)
    return (hidden_wide + mixed).astype(jnp.bfloat16)


def solution(mesh):
    expert_ranks, tensor_ranks = mesh.shape["expert"], mesh.shape["tensor"]
    paired = tensor_ranks == 4 and 2 * expert_ranks == E
    return jax.shard_map(
        paired_shards if paired else shards,
        mesh=mesh,
        in_specs=(
            P(("groups", "expert", "tensor"), None),
            P(("groups", "expert"), "tensor"),
            P(),
            P(),
            P(("groups", "expert", "tensor"), None),
            P(None, ("expert", "tensor")),
            P(None, ("expert", "tensor")),
            P(("expert", "tensor"), None),
        ),
        out_specs=P(("groups", "expert", "tensor"), None),
        check_vma=False,
    )
```
